32 devices in a mesh: dp: 8 (over z, x), mp: 4 (over y, core).
Axes of the slice: x: 2, y: 2, z: 4, core: 2. Of those that a mesh axis runs over, the one named last changes fastest.
Arguments:
- images: bfloat16 [4096, 768], P(('dp', 'mp')), may hold values from -64 to 64
- texts: bfloat16 [4096, 768], P(('dp', 'mp')), may hold values from -64 to 64
- log_scale: float32 [1], replicated, may hold values from 2.5 to 3.5
- bias: float32 [1], replicated, may hold values from -6 to -3
Outputs:
- row_loss: float32 [4096], P(('dp', 'mp'))
- col_loss: float32 [4096], P(('dp', 'mp'))
The draws below stay inside these ranges and needn't reach their ends.
All inputs are finite; a program needn't handle non-finite values.
Results may differ from the reference program's by a relative error of at most 0.0008.
Values may be sent and summed in bfloat16 or wider, within the bound.
No kernel may reach another device: no remote copies, remote signals or barrier semaphores. Data moves between devices by JAX's collectives and lax.ppermute only.
A program may use at most 64 MiB of HBM per device.

```python
import math
import jax
import jax.numpy as jnp
from jax import lax

E = 768
TOK_DEV = 512
TOKENS = 4096
N_DP = 8


def embedding_pair(key):
    groups_count = max(TOKENS // 256, 2)
    subkeys = jax.random.split(jax.random.fold_in(key, 4409), 9)
    labels = jax.random.randint(subkeys[0], (TOKENS,), 0, groups_count)
    centers = jax.random.normal(subkeys[1], (groups_count, E), jnp.float32)
    shared = centers[labels]
    own_part = jax.random.normal(subkeys[2], (TOKENS, E), jnp.float32)
    other_part = jax.random.normal(subkeys[3], (TOKENS, E), jnp.float32)
    strength = jax.random.uniform(subkeys[4], (groups_count,), jnp.float32, 0.3, 0.5)
    match_share = jax.random.uniform(subkeys[5], (TOKENS, 1), jnp.float32, 0.45, 0.55)
    lowest_scale = 0.5
    highest_scale = 4.0
    cluster_mix = strength[labels][:, None]
    image_dir = jnp.sqrt(cluster_mix) * shared + jnp.sqrt(1.0 - cluster_mix) * own_part
    text_noise = match_share * own_part + jnp.sqrt(1.0 - match_share * match_share) * other_part
    text_dir = jnp.sqrt(cluster_mix) * shared + jnp.sqrt(1.0 - cluster_mix) * text_noise
    image_scale = jnp.exp(jax.random.uniform(subkeys[7], (TOKENS, 1), jnp.float32, math.log(lowest_scale), math.log(highest_scale)))
    text_scale = jnp.exp(jax.random.uniform(subkeys[8], (TOKENS, 1), jnp.float32, math.log(lowest_scale), math.log(highest_scale)))
    images = jnp.clip(image_scale * image_dir, -64.0, 64.0)
    texts = jnp.clip(text_scale * text_dir, -64.0, 64.0)
    return (images, texts)


def draw_images(key, part):
    return embedding_pair(key)[0].astype(jnp.bfloat16)


def draw_texts(key, part):
    return embedding_pair(key)[1].astype(jnp.bfloat16)


def setup_inputs(seed: int = 0) -> dict:
    keys = jax.random.split(jax.random.key(seed), 5)
    return {
        "images": draw_images(jax.random.fold_in(keys[4], 71), 0),
        "texts": draw_texts(jax.random.fold_in(keys[4], 71), 0),
        "log_scale": jnp.clip(jax.random.uniform(keys[2], (1,), jnp.float32, 2.5, 3.5), 2.5, 3.5),
        "bias": jnp.clip(jax.random.uniform(keys[3], (1,), jnp.float32, -6.0, -3.0), -6.0, -3.0),
    }


EPSILON = 1e-06

def unit_rows(values):
    widened = values.astype(jnp.float32)
    inverse = lax.rsqrt(lax.optimization_barrier(jnp.sum(widened * widened, axis=1, keepdims=True)) + EPSILON)
    return (widened * inverse).astype(jnp.bfloat16)

def reference(images, texts, log_scale, bias):
    img_unit = unit_rows(images).astype(jnp.float32)
    txt_unit = unit_rows(texts).astype(jnp.float32)
    logit_scale = jnp.exp(log_scale[0])
    offset = bias[0]
    columns = lax.broadcasted_iota(jnp.int32, (TOK_DEV, TOKENS), 1)
    local_rows = lax.broadcasted_iota(jnp.int32, (TOK_DEV, TOKENS), 0)

    def block_step(col_total, block_index):
        first_row = (block_index * TOK_DEV).astype(jnp.int32)
        image_rows = lax.dynamic_slice_in_dim(img_unit, first_row, TOK_DEV, 0)
        scores = lax.dot_general(image_rows, txt_unit, (((1,), (1,)), ((), ())), precision=lax.Precision.HIGHEST, preferred_element_type=jnp.float32)
        logits = logit_scale * scores + offset
        matched = columns == local_rows + first_row
        losses = jax.nn.softplus(jnp.where(matched, -logits, logits))
        return (col_total + lax.optimization_barrier(jnp.sum(losses, axis=0)), lax.optimization_barrier(jnp.sum(losses, axis=1)))
    col_total, row_parts = lax.scan(block_step, jnp.zeros((TOKENS,), jnp.float32), jnp.arange(N_DP, dtype=jnp.int32))
    row_loss = row_parts.reshape(TOKENS) / TOK_DEV
    col_loss = col_total / TOK_DEV
    return (row_loss, col_loss)
```

```python
import math

import jax
import jax.numpy as jnp
from jax import lax
from jax.experimental import pallas as pl
from jax.experimental.pallas import tpu as pltpu
from jax.sharding import PartitionSpec as P

TOK_DEV = 512

EPSILON = 1e-06

AXES = ("dp", "mp")


VMEM = pl.BlockSpec(memory_space=pltpu.VMEM)
SMEM = pl.BlockSpec(memory_space=pltpu.SMEM)


def unit_rows(values):
    widened = values.astype(jnp.float32)
    inverse = lax.rsqrt(jnp.sum(widened * widened, axis=1, keepdims=True) + EPSILON)
    return (widened * inverse).astype(jnp.bfloat16)


def softplus(logits):
    grown = jnp.exp(logits)
    series = grown * (1.0 + grown * (-1.0 / 2 + grown * (1.0 / 3 - grown * (1.0 / 4))))
    return jnp.where(grown < 1.0 / 32, series, jnp.log(1.0 + grown))


def pair_kernel(n_images, n_texts, log_scale, bias, *refs):
    images = refs[:n_images]
    texts = refs[n_images : n_images + n_texts]
    row_out, col_out, text_unit = refs[n_images + n_texts :]
    rows = images[0].shape[0]
    logit_scale = jnp.exp(jnp.full((1, 1), log_scale[0], jnp.float32))
    offset = bias[0]
    for j in range(n_texts):
        text_unit[pl.ds(j * rows, rows), :] = unit_rows(texts[j][...])
    col_parts = [None] * n_texts
    for i in range(n_images):
        unit = unit_rows(images[i][...])
        row_part = None
        for j in range(n_texts):
            scores = lax.dot_general(
                unit,
                text_unit[pl.ds(j * rows, rows), :],
                (((1,), (1,)), ((), ())),
                preferred_element_type=jnp.float32,
            )
            logits = logit_scale * scores + offset
            if i == 0 and j == 0:
                down = lax.broadcasted_iota(jnp.int32, logits.shape, 0)
                across = lax.broadcasted_iota(jnp.int32, logits.shape, 1)
                logits = jnp.where(down == across, -logits, logits)
            losses = softplus(logits)
            row_part = losses if row_part is None else row_part + losses
            part = jnp.sum(losses.reshape(rows // 8, 8, rows), axis=0)
            col_parts[j] = part if col_parts[j] is None else col_parts[j] + part
        row_out[i : i + 1, :] = jnp.sum(row_part.T, axis=0, keepdims=True)
    for j in range(n_texts):
        col_out[j : j + 1, :] = jnp.sum(col_parts[j], axis=0, keepdims=True)


def pair_sums(log_scale, bias, images, texts):
    rows, width = images[0].shape
    n_images, n_texts = len(images), len(texts)
    pairs = n_images * n_texts * rows * rows
    return pl.pallas_call(
        lambda *refs: pair_kernel(n_images, n_texts, *refs),
        out_shape=(
            jax.ShapeDtypeStruct((n_images, rows), jnp.float32),
            jax.ShapeDtypeStruct((n_texts, rows), jnp.float32),
        ),
        in_specs=[SMEM, SMEM] + [VMEM] * (n_images + n_texts),
        out_specs=(VMEM, VMEM),
        scratch_shapes=[pltpu.VMEM((n_texts * rows, width), jnp.bfloat16)],
        cost_estimate=pl.CostEstimate(
            flops=2 * pairs * width,
            bytes_accessed=(n_images + n_texts) * rows * width * 2,
            transcendentals=2 * pairs,
        ),
        name="pair_sums",
    )(log_scale, bias, *images, *texts)


def solution(mesh):
    n_dp, n_mp = mesh.shape["dp"], mesh.shape["mp"]
    n_devices = n_dp * n_mp
    bits = [1 << k for k in range(int(math.log2(n_devices)))]
    mp_bits = [b for b in bits if b < n_mp]
    dp_bits = [b for b in bits if b >= n_mp]
    text_bits = dp_bits[0::2][::-1] + mp_bits[0::2][::-1]
    image_bits = dp_bits[1::2][::-1] + mp_bits[1::2][::-1]

    def swap(value, bit):
        return lax.ppermute(value, AXES, [(d, d ^ bit) for d in range(n_devices)])

    def gather(own, order):
        blocks = [own]
        for bit in order:
            blocks = blocks + [swap(block, bit) for block in blocks]
        return blocks

    def scatter_sum(parts, order):
        for bit in reversed(order):
            half = parts.shape[0] // 2
            parts = parts[:half] + swap(parts[half:], bit)
        return parts

    def local(images, texts, log_scale, bias):
        image_blocks = gather(images, image_bits)
        text_blocks = gather(texts, text_bits)
        row_parts, col_parts = pair_sums(log_scale, bias, image_blocks, text_blocks)
        row_sums = scatter_sum(row_parts, image_bits)
        col_sums = scatter_sum(col_parts, text_bits)
        return (row_sums[0] / TOK_DEV, col_sums[0] / TOK_DEV)

    placed = (P(AXES, None), P(AXES, None), P(), P())
    return jax.shard_map(
        local,
        mesh=mesh,
        in_specs=placed,
        out_specs=(P(AXES), P(AXES)),
        check_vma=False,
    )
```

```python
import math

import jax
import jax.numpy as jnp
from jax import lax
from jax.experimental import pallas as pl
from jax.experimental.pallas import tpu as pltpu
from jax.sharding import PartitionSpec as P

TOK_DEV = 512

EPSILON = 1e-06

AXES = ("dp", "mp")


VMEM = pl.BlockSpec(memory_space=pltpu.VMEM)
SMEM = pl.BlockSpec(memory_space=pltpu.SMEM)


def unit_rows(values):
    widened = values.astype(jnp.float32)
    inverse = lax.rsqrt(jnp.sum(widened * widened, axis=1, keepdims=True) + EPSILON)
    return (widened * inverse).astype(jnp.bfloat16)


def softplus(logits):
    grown = jnp.exp(logits)
    series = grown * (1.0 + grown * (-1.0 / 2 + grown * (1.0 / 3 - grown * (1.0 / 4))))
    return jnp.where(grown < 1.0 / 32, series, jnp.log(1.0 + grown))


def pair_losses(scalars, image_unit, text_unit, own_pairs=False):
    logit_scale, offset = scalars
    scores = lax.dot_general(
        image_unit, text_unit, (((1,), (1,)), ((), ())), preferred_element_type=jnp.float32
    )
    logits = logit_scale * scores + offset
    if own_pairs:
        down = lax.broadcasted_iota(jnp.int32, logits.shape, 0)
        across = lax.broadcasted_iota(jnp.int32, logits.shape, 1)
        logits = jnp.where(down == across, -logits, logits)
    return softplus(logits)


def row_line(losses):
    rows = losses.shape[0]
    lanes = [losses[:, k : k + rows] for k in range(0, losses.shape[1], rows)]
    return jnp.sum(sum(lanes[1:], lanes[0]).T, axis=0, keepdims=True)


def col_tile(losses):
    return jnp.sum(losses.reshape(losses.shape[0] // 8, 8, losses.shape[1]), axis=0)


def col_lines(tile, rows):
    line = jnp.sum(tile, axis=0, keepdims=True)
    return [line[:, k : k + rows] for k in range(0, line.shape[1], rows)]


def own_kernel(log_scale, bias, image, text, scalars, image_unit, text_unit):
    line = scalars.shape[1]
    scalars[0:1, :] = jnp.broadcast_to(jnp.exp(log_scale[...]), (1, line))
    scalars[1:2, :] = jnp.broadcast_to(bias[...], (1, line))
    image_unit[...] = unit_rows(image[...])
    text_unit[...] = unit_rows(text[...])


def loss_scalars(ref):
    return ref[0:1, 0:1], ref[1:2, 0:1]


def early_kernel(n_images, n_texts, scalar_ref, own_image, own_text, *refs):
    images = (own_image,) + refs[: n_images - 1]
    texts = (own_text,) + refs[n_images - 1 : n_images + n_texts - 2]
    row_out, col_out, image_unit, text_unit = refs[n_images + n_texts - 2 :]
    rows = own_image.shape[0]
    scalars = loss_scalars(scalar_ref)
    for j in range(n_texts):
        unit = unit_rows(texts[j][...]) if j else own_text[...]
        text_unit[pl.ds(j * rows, rows), :] = unit
    col_sum = None
    for i in range(n_images):
        unit = unit_rows(images[i][...]) if i else own_image[...]
        image_unit[pl.ds(i * rows, rows), :] = unit
        losses = pair_losses(scalars, unit, text_unit[...], own_pairs=i == 0)
        row_out[i : i + 1, :] = row_line(losses)
        tile = col_tile(losses)
        col_sum = tile if col_sum is None else col_sum + tile
    for j, line in enumerate(col_lines(col_sum, rows)):
        col_out[j : j + 1, :] = line


def late_kernel(n_images, n_texts, core, scalar_ref, *refs):
    early_rows, early_cols, image_unit, text_unit = refs[:4]
    images = refs[4 : 4 + n_images]
    texts = refs[4 + n_images : 4 + n_images + n_texts]
    send, keep, row_total, col_total, late_text = refs[4 + n_images + n_texts :]
    rows = images[0].shape[0]
    n_early_images, n_early_texts = early_rows.shape[0], early_cols.shape[0]
    scalars = loss_scalars(scalar_ref)
    for j in range(n_texts):
        late_text[pl.ds(j * rows, rows), :] = unit_rows(texts[j][...])
    late_sum = None
    for i in range(n_early_images):
        losses = pair_losses(scalars, image_unit[pl.ds(i * rows, rows), :], late_text[...])
        row_total[i : i + 1, :] = early_rows[i : i + 1, :] + row_line(losses)
        tile = col_tile(losses)
        late_sum = tile if late_sum is None else late_sum + tile
    early_sum = None
    for i in range(n_images):
        unit = unit_rows(images[i][...])
        losses = pair_losses(scalars, unit, late_text[...])
        late_sum = late_sum + col_tile(losses)
        line = row_line(losses)
        losses = pair_losses(scalars, unit, text_unit[...])
        tile = col_tile(losses)
        early_sum = tile if early_sum is None else early_sum + tile
        k = n_early_images + i
        row_total[k : k + 1, :] = line + row_line(losses)
    for j, line in enumerate(col_lines(early_sum, rows)):
        col_total[j : j + 1, :] = early_cols[j : j + 1, :] + line
    for j, line in enumerate(col_lines(late_sum, rows)):
        k = n_early_texts + j
        col_total[k : k + 1, :] = line
    send[...] = jnp.zeros_like(send)
    keep[...] = jnp.zeros_like(keep)
    row_units, col_units = row_total.shape[0] // 2, col_total.shape[0]

    @pl.when(core[0] == 0)
    def _():
        for m in range(row_units):
            keep[m] = row_total[2 * m : 2 * m + 2, :] * (1.0 / TOK_DEV)
        for m in range(col_units):
            send[m, 1:2] = col_total[m : m + 1, :] * (1.0 / TOK_DEV)

    @pl.when(core[0] != 0)
    def _():
        for m in range(row_units):
            for k in range(2):
                send[m, k : k + 1] = row_total[2 * m + 1 - k : 2 * m + 2 - k, :] * (1.0 / TOK_DEV)
        for m in range(col_units):
            keep[m, 0:1] = col_total[m : m + 1, :] * (1.0 / TOK_DEV)


def estimate(pairs, width, blocks, rows):
    return pl.CostEstimate(
        flops=2 * pairs * width,
        bytes_accessed=blocks * rows * width * 2,
        transcendentals=2 * pairs,
    )


def own_units(log_scale, bias, image, text):
    unit = jax.ShapeDtypeStruct(image.shape, jnp.bfloat16)
    return pl.pallas_call(
        own_kernel,
        out_shape=(jax.ShapeDtypeStruct((2, 128), jnp.float32), unit, unit),
        in_specs=[VMEM] * 4,
        out_specs=(VMEM,) * 3,
        cost_estimate=pl.CostEstimate(
            flops=8 * image.size, bytes_accessed=8 * image.size, transcendentals=0
        ),
        compiler_params=pltpu.CompilerParams(vmem_limit_bytes=16 << 20),
        name="own_units",
    )(log_scale, bias, image, text)


def early_sums(scalars, own_image, own_text, images, texts):
    rows, width = own_image.shape
    n_images, n_texts = len(images) + 1, len(texts) + 1
    return pl.pallas_call(
        lambda *refs: early_kernel(n_images, n_texts, *refs),
        out_shape=(
            jax.ShapeDtypeStruct((n_images, rows), jnp.float32),
            jax.ShapeDtypeStruct((n_texts, rows), jnp.float32),
            jax.ShapeDtypeStruct((n_images * rows, width), jnp.bfloat16),
            jax.ShapeDtypeStruct((n_texts * rows, width), jnp.bfloat16),
        ),
        in_specs=[VMEM] * (1 + n_images + n_texts),
        out_specs=(VMEM,) * 4,
        cost_estimate=estimate(n_images * n_texts * rows * rows, width, n_images + n_texts, rows),
        compiler_params=pltpu.CompilerParams(vmem_limit_bytes=16 << 20),
        name="early_sums",
    )(scalars, own_image, own_text, *images, *texts)


def late_sums(core, scalars, early, images, texts):
    rows, width = images[0].shape
    n_images, n_texts = len(images), len(texts)
    all_images = early[0].shape[0] + n_images
    all_texts = early[1].shape[0] + n_texts
    pairs = (all_images * all_texts - early[0].shape[0] * early[1].shape[0]) * rows * rows
    units = max(all_images // 2, all_texts)
    return pl.pallas_call(
        lambda *refs: late_kernel(n_images, n_texts, *refs),
        out_shape=(jax.ShapeDtypeStruct((units, 2, rows), jnp.float32),) * 2,
        in_specs=[SMEM] + [VMEM] * (5 + n_images + n_texts),
        out_specs=(VMEM, VMEM),
        scratch_shapes=[
            pltpu.VMEM((all_images, rows), jnp.float32),
            pltpu.VMEM((all_texts, rows), jnp.float32),
            pltpu.VMEM((n_texts * rows, width), jnp.bfloat16),
        ],
        cost_estimate=estimate(pairs, width, all_images + all_texts, rows),
        compiler_params=pltpu.CompilerParams(vmem_limit_bytes=16 << 20),
        name="late_sums",
    )(core, scalars, *early, *images, *texts)


def solution(mesh):
    n_devices = mesh.shape["dp"] * mesh.shape["mp"]
    bits = [1 << k for k in range(int(math.log2(n_devices)))]
    dp_bits = [b for b in bits if b >= mesh.shape["mp"]]
    split = dp_bits[0::2] + dp_bits[1::2]
    text_bits = sorted(split[: len(bits) // 2], reverse=True)
    image_bits = sorted(set(bits) - set(text_bits), reverse=True)
    core_bit, link_bits = image_bits[-1], image_bits[:-1]

    def masks_of(order):
        masks = [0]
        for bit in order:
            masks = masks + [mask | bit for mask in masks]
        return masks

    image_masks = sorted(masks_of(link_bits), key=lambda m: m.bit_count())
    text_masks = sorted(masks_of(text_bits), key=lambda m: m.bit_count())

    def move(value, partner):
        pairs = [(d, partner(d)) for d in range(n_devices) if partner(d) != d]
        return lax.ppermute(value, AXES, pairs)

    def swap(value, bit):
        return move(value, lambda d: d ^ bit)

    def gather(own, order):
        blocks = {0: own}
        for bit in order:
            for mask, block in list(blocks.items()):
                blocks[mask | bit] = swap(block, bit)
        return blocks

    def losses(images, texts, log_scale, bias):
        scalars, own_image, own_text = own_units(
            log_scale.reshape(1, 1), bias.reshape(1, 1), images, texts
        )
        core = (lax.axis_index("mp") & 1).astype(jnp.int32)
        image_blocks = gather(images, link_bits)
        text_blocks = gather(texts, text_bits)
        paired = {m: swap(b, core_bit) for m, b in image_blocks.items()}
        early_masks = [m for m in image_masks if m.bit_count() < 2]
        late_masks = [m for m in image_masks if m.bit_count() >= 2]
        both = lambda masks: [b for m in masks for b in (image_blocks[m], paired[m])]
        early_texts = [text_blocks[m] for m in text_masks if m.bit_count() < 2]
        late_texts = [text_blocks[m] for m in text_masks if m.bit_count() >= 2]
        early = early_sums(
            scalars, own_image, own_text, both(early_masks)[1:], early_texts[1:]
        )
        send, keep = late_sums(
            core.reshape(1), scalars, early, both(late_masks), late_texts
        )
        merged = keep + swap(send, core_bit)
        total = merged[0]
        for k in reversed(range(1, merged.shape[0])):
            row_mask = image_masks[k] if k < len(image_masks) else 0
            col_mask = text_masks[k] if k < len(text_masks) else 0
            total = total + move(merged[k], lambda d: d ^ (col_mask if d & core_bit else row_mask))
        other = swap(total[1:2], core_bit)
        on_rows = core == 0
        own = total[0:1]
        row_loss = jnp.where(on_rows, own, other).reshape(-1)
        col_loss = jnp.where(on_rows, other, own).reshape(-1)
        return row_loss, col_loss

    placed = (P(AXES, None), P(AXES, None), P(), P())
    return jax.shard_map(
        losses,
        mesh=mesh,
        in_specs=placed,
        out_specs=(P(AXES), P(AXES)),
        check_vma=False,
    )
```

```python
import math

import jax
import jax.numpy as jnp
from jax import lax
from jax.experimental import pallas as pl
from jax.experimental.pallas import tpu as pltpu
from jax.sharding import PartitionSpec as P

TOK_DEV = 512

EPSILON = 1e-06

AXES = ("dp", "mp")


VMEM = pl.BlockSpec(memory_space=pltpu.VMEM)
SMEM = pl.BlockSpec(memory_space=pltpu.SMEM)


def unit_rows(values):
    widened = values.astype(jnp.float32)
    inverse = lax.rsqrt(jnp.sum(widened * widened, axis=1, keepdims=True) + EPSILON)
    return (widened * inverse).astype(jnp.bfloat16)


def softplus(logits):
    grown = jnp.exp(logits)
    series = grown * (1.0 + grown * (-1.0 / 2 + grown * (1.0 / 3 - grown * (1.0 / 4))))
    return jnp.where(grown < 1.0 / 32, series, jnp.log(1.0 + grown))


def pair_losses(scalars, image_unit, text_unit, own_pairs=False):
    logit_scale, offset = scalars
    scores = lax.dot_general(
        image_unit, text_unit, (((1,), (1,)), ((), ())), preferred_element_type=jnp.float32
    )
    logits = logit_scale * scores + offset
    if own_pairs:
        down = lax.broadcasted_iota(jnp.int32, logits.shape, 0)
        across = lax.broadcasted_iota(jnp.int32, logits.shape, 1)
        logits = jnp.where(down == across, -logits, logits)
    return softplus(logits)


def row_line(losses):
    rows = losses.shape[0]
    lanes = [losses[:, k : k + rows] for k in range(0, losses.shape[1], rows)]
    return jnp.sum(sum(lanes[1:], lanes[0]).T, axis=0, keepdims=True)


def col_tile(losses):
    return jnp.sum(losses.reshape(losses.shape[0] // 8, 8, losses.shape[1]), axis=0)


def col_lines(tile, rows):
    line = jnp.sum(tile, axis=0, keepdims=True)
    return [line[:, k : k + rows] for k in range(0, line.shape[1], rows)]


def own_kernel(log_scale, bias, image, text, scalars, image_unit, text_unit):
    line = scalars.shape[1]
    scalars[0:1, :] = jnp.broadcast_to(jnp.exp(log_scale[...]), (1, line))
    scalars[1:2, :] = jnp.broadcast_to(bias[...], (1, line))
    image_unit[...] = unit_rows(image[...])
    text_unit[...] = unit_rows(text[...])


def loss_scalars(ref):
    return ref[0:1, 0:1], ref[1:2, 0:1]


def early_kernel(n_images, n_texts, scalar_ref, own_image, own_text, *refs):
    images = (own_image,) + refs[: n_images - 1]
    texts = (own_text,) + refs[n_images - 1 : n_images + n_texts - 2]
    row_out, col_out, image_unit, text_unit = refs[n_images + n_texts - 2 :]
    rows = own_image.shape[0]
    scalars = loss_scalars(scalar_ref)
    for j in range(n_texts):
        unit = unit_rows(texts[j][...]) if j else own_text[...]
        text_unit[pl.ds(j * rows, rows), :] = unit
    col_sum = None
    for i in range(n_images):
        unit = unit_rows(images[i][...]) if i else own_image[...]
        image_unit[pl.ds(i * rows, rows), :] = unit
        losses = pair_losses(scalars, unit, text_unit[...], own_pairs=i == 0)
        row_out[i : i + 1, :] = row_line(losses)
        tile = col_tile(losses)
        col_sum = tile if col_sum is None else col_sum + tile
    for j, line in enumerate(col_lines(col_sum, rows)):
        col_out[j : j + 1, :] = line


def late_kernel(n_images, n_texts, core, scalar_ref, *refs):
    early_rows, early_cols, image_unit, text_unit = refs[:4]
    images = refs[4 : 4 + n_images]
    texts = refs[4 + n_images : 4 + n_images + n_texts]
    send, keep, row_total, col_total, late_text = refs[4 + n_images + n_texts :]
    rows = images[0].shape[0]
    n_early_images, n_early_texts = early_rows.shape[0], early_cols.shape[0]
    scalars = loss_scalars(scalar_ref)
    for j in range(n_texts):
        late_text[pl.ds(j * rows, rows), :] = unit_rows(texts[j][...])
    late_sum = None
    for i in range(n_early_images):
        losses = pair_losses(scalars, image_unit[pl.ds(i * rows, rows), :], late_text[...])
        row_total[i : i + 1, :] = early_rows[i : i + 1, :] + row_line(losses)
        tile = col_tile(losses)
        late_sum = tile if late_sum is None else late_sum + tile
    early_sum = None
    for i in range(n_images):
        unit = unit_rows(images[i][...])
        losses = pair_losses(scalars, unit, late_text[...])
        late_sum = late_sum + col_tile(losses)
        line = row_line(losses)
        losses = pair_losses(scalars, unit, text_unit[...])
        tile = col_tile(losses)
        early_sum = tile if early_sum is None else early_sum + tile
        k = n_early_images + i
        row_total[k : k + 1, :] = line + row_line(losses)
    for j, line in enumerate(col_lines(early_sum, rows)):
        col_total[j : j + 1, :] = early_cols[j : j + 1, :] + line
    for j, line in enumerate(col_lines(late_sum, rows)):
        k = n_early_texts + j
        col_total[k : k + 1, :] = line
    send[...] = jnp.zeros_like(send)
    keep[...] = jnp.zeros_like(keep)
    row_units, col_units = row_total.shape[0] // 2, col_total.shape[0]

    @pl.when(core[0] == 0)
    def _():
        for m in range(row_units):
            keep[m] = row_total[2 * m : 2 * m + 2, :] * (1.0 / TOK_DEV)
        for m in range(col_units):
            send[m, 1:2] = col_total[m : m + 1, :] * (1.0 / TOK_DEV)

    @pl.when(core[0] != 0)
    def _():
        for m in range(row_units):
            for k in range(2):
                send[m, k : k + 1] = row_total[2 * m + 1 - k : 2 * m + 2 - k, :] * (1.0 / TOK_DEV)
        for m in range(col_units):
            keep[m, 0:1] = col_total[m : m + 1, :] * (1.0 / TOK_DEV)


def estimate(pairs, width, blocks, rows):
    return pl.CostEstimate(
        flops=2 * pairs * width,
        bytes_accessed=blocks * rows * width * 2,
        transcendentals=2 * pairs,
    )


def own_units(log_scale, bias, image, text):
    unit = jax.ShapeDtypeStruct(image.shape, jnp.bfloat16)
    return pl.pallas_call(
        own_kernel,
        out_shape=(jax.ShapeDtypeStruct((2, 128), jnp.float32), unit, unit),
        in_specs=[VMEM] * 4,
        out_specs=(VMEM,) * 3,
        cost_estimate=pl.CostEstimate(
            flops=8 * image.size, bytes_accessed=8 * image.size, transcendentals=0
        ),
        compiler_params=pltpu.CompilerParams(vmem_limit_bytes=16 << 20),
        name="own_units",
    )(log_scale, bias, image, text)


def early_sums(scalars, own_image, own_text, images, texts):
    rows, width = own_image.shape
    n_images, n_texts = len(images) + 1, len(texts) + 1
    return pl.pallas_call(
        lambda *refs: early_kernel(n_images, n_texts, *refs),
        out_shape=(
            jax.ShapeDtypeStruct((n_images, rows), jnp.float32),
            jax.ShapeDtypeStruct((n_texts, rows), jnp.float32),
            jax.ShapeDtypeStruct((n_images * rows, width), jnp.bfloat16),
            jax.ShapeDtypeStruct((n_texts * rows, width), jnp.bfloat16),
        ),
        in_specs=[VMEM] * (1 + n_images + n_texts),
        out_specs=(VMEM,) * 4,
        cost_estimate=estimate(n_images * n_texts * rows * rows, width, n_images + n_texts, rows),
        compiler_params=pltpu.CompilerParams(vmem_limit_bytes=16 << 20),
        name="early_sums",
    )(scalars, own_image, own_text, *images, *texts)


def late_sums(core, scalars, early, images, texts):
    rows, width = images[0].shape
    n_images, n_texts = len(images), len(texts)
    all_images = early[0].shape[0] + n_images
    all_texts = early[1].shape[0] + n_texts
    pairs = (all_images * all_texts - early[0].shape[0] * early[1].shape[0]) * rows * rows
    units = max(all_images // 2, all_texts)
    return pl.pallas_call(
        lambda *refs: late_kernel(n_images, n_texts, *refs),
        out_shape=(jax.ShapeDtypeStruct((units, 2, rows), jnp.float32),) * 2,
        in_specs=[SMEM] + [VMEM] * (5 + n_images + n_texts),
        out_specs=(VMEM, VMEM),
        scratch_shapes=[
            pltpu.VMEM((all_images, rows), jnp.float32),
            pltpu.VMEM((all_texts, rows), jnp.float32),
            pltpu.VMEM((n_texts * rows, width), jnp.bfloat16),
        ],
        cost_estimate=estimate(pairs, width, all_images + all_texts, rows),
        compiler_params=pltpu.CompilerParams(vmem_limit_bytes=16 << 20),
        name="late_sums",
    )(core, scalars, *early, *images, *texts)


def solution(mesh):
    n_devices = mesh.shape["dp"] * mesh.shape["mp"]
    bits = [1 << k for k in range(int(math.log2(n_devices)))]
    dp_bits = [b for b in bits if b >= mesh.shape["mp"]]
    split = dp_bits[0::2] + dp_bits[1::2]
    text_bits = sorted(split[: len(bits) // 2], reverse=True)
    image_bits = sorted(set(bits) - set(text_bits), reverse=True)
    core_bit, link_bits = image_bits[-1], image_bits[:-1]

    def masks_of(order):
        masks = [0]
        for bit in order:
            masks = masks + [mask | bit for mask in masks]
        return masks

    image_masks = sorted(masks_of(link_bits), key=lambda m: m.bit_count())
    text_masks = sorted(masks_of(text_bits), key=lambda m: m.bit_count())

    def move(value, partner):
        pairs = [(d, partner(d)) for d in range(n_devices) if partner(d) != d]
        return lax.ppermute(value, AXES, pairs)

    def swap(value, bit):
        return move(value, lambda d: d ^ bit)

    def gather(own, order):
        blocks = {0: own}
        for bit in order:
            for mask, block in list(blocks.items()):
                blocks[mask | bit] = swap(block, bit)
        return blocks

    def losses(images, texts, log_scale, bias):
        scalars, own_image, own_text = own_units(
            log_scale.reshape(1, 1), bias.reshape(1, 1), images, texts
        )
        core = (lax.axis_index("mp") & 1).astype(jnp.int32)
        image_blocks = {m: move(images, lambda d: d ^ m) for m in image_masks if m}
        image_blocks[0] = images
        text_blocks = gather(texts, text_bits)
        paired = {m: swap(b, core_bit) for m, b in image_blocks.items()}
        early_masks = [m for m in image_masks if m.bit_count() < 2]
        late_masks = [m for m in image_masks if m.bit_count() >= 2]
        both = lambda masks: [b for m in masks for b in (image_blocks[m], paired[m])]
        early_texts = [text_blocks[m] for m in text_masks if m.bit_count() < 2]
        late_texts = [text_blocks[m] for m in text_masks if m.bit_count() >= 2]
        early = early_sums(
            scalars, own_image, own_text, both(early_masks)[1:], early_texts[1:]
        )
        send, keep = late_sums(
            core.reshape(1), scalars, early, both(late_masks), late_texts
        )
        merged = keep + swap(send, core_bit)
        total = merged[0]
        for k in range(1, merged.shape[0]):
            row_mask = image_masks[k] if k < len(image_masks) else 0
            col_mask = text_masks[k] if k < len(text_masks) else 0
            total = total + move(merged[k], lambda d: d ^ (col_mask if d & core_bit else row_mask))
        other = swap(total[1:2], core_bit)
        on_rows = core == 0
        own = total[0:1]
        row_loss = jnp.where(on_rows, own, other).reshape(-1)
        col_loss = jnp.where(on_rows, other, own).reshape(-1)
        return row_loss, col_loss

    placed = (P(AXES, None), P(AXES, None), P(), P())
    return jax.shard_map(
        losses,
        mesh=mesh,
        in_specs=placed,
        out_specs=(P(AXES), P(AXES)),
        check_vma=False,
    )
```

```python
import math

import jax
import jax.numpy as jnp
from jax import lax
from jax.experimental import pallas as pl
from jax.experimental.pallas import tpu as pltpu
from jax.sharding import PartitionSpec as P

TOK_DEV = 512

EPSILON = 1e-06

LOG2_E = math.log2(math.e)

AXES = ("dp", "mp")


VMEM = pl.BlockSpec(memory_space=pltpu.VMEM)
SMEM = pl.BlockSpec(memory_space=pltpu.SMEM)


def unit_rows(values):
    widened = values.astype(jnp.float32)
    inverse = lax.rsqrt(jnp.sum(widened * widened, axis=1, keepdims=True) + EPSILON)
    return (widened * inverse).astype(jnp.bfloat16)


def softplus(grown):
    series = grown * (1.0 + grown * (-1.0 / 2 + grown * (1.0 / 3)))
    return jnp.where(grown < 1.0 / 64, series, jnp.log(1.0 + grown))


def pair_losses(scalars, image_unit, text_unit, own_pairs=False):
    logit_scale, offset = scalars
    scores = lax.dot_general(
        image_unit, text_unit, (((1,), (1,)), ((), ())), preferred_element_type=jnp.float32
    )
    logits = logit_scale * scores + offset
    if own_pairs:
        down = lax.broadcasted_iota(jnp.int32, logits.shape, 0)
        across = lax.broadcasted_iota(jnp.int32, logits.shape, 1)
        logits = jnp.where(down == across, -logits, logits)
    return softplus(jnp.exp2(logits))


def row_line(losses):
    rows = losses.shape[0]
    lanes = [losses[:, k : k + rows] for k in range(0, losses.shape[1], rows)]
    return jnp.sum(sum(lanes[1:], lanes[0]).T, axis=0, keepdims=True)


def col_tile(losses):
    return jnp.sum(losses.reshape(losses.shape[0] // 8, 8, losses.shape[1]), axis=0)


def col_lines(tile, rows):
    line = jnp.sum(tile, axis=0, keepdims=True)
    return [line[:, k : k + rows] for k in range(0, line.shape[1], rows)]


def own_kernel(log_scale, bias, image, text, scalars, image_unit, text_unit):
    line = scalars.shape[1]
    scalars[0:1, :] = jnp.broadcast_to(jnp.exp(log_scale[...]) * LOG2_E, (1, line))
    scalars[1:2, :] = jnp.broadcast_to(bias[...] * LOG2_E, (1, line))
    image_unit[...] = unit_rows(image[...])
    text_unit[...] = unit_rows(text[...])


def loss_scalars(ref):
    return ref[0:1, 0:1], ref[1:2, 0:1]


def early_kernel(n_images, n_texts, scalar_ref, own_image, own_text, *refs):
    images = (own_image,) + refs[: n_images - 1]
    texts = (own_text,) + refs[n_images - 1 : n_images + n_texts - 2]
    row_out, col_out, image_unit, text_unit = refs[n_images + n_texts - 2 :]
    rows = own_image.shape[0]
    scalars = loss_scalars(scalar_ref)
    for j in range(n_texts):
        unit = unit_rows(texts[j][...]) if j else own_text[...]
        text_unit[pl.ds(j * rows, rows), :] = unit
    col_sum = None
    for i in range(n_images):
        unit = unit_rows(images[i][...]) if i else own_image[...]
        image_unit[pl.ds(i * rows, rows), :] = unit
        losses = pair_losses(scalars, unit, text_unit[...], own_pairs=i == 0)
        row_out[i : i + 1, :] = row_line(losses)
        tile = col_tile(losses)
        col_sum = tile if col_sum is None else col_sum + tile
    for j, line in enumerate(col_lines(col_sum, rows)):
        col_out[j : j + 1, :] = line


def late_kernel(n_images, n_texts, core, scalar_ref, *refs):
    early_rows, early_cols, image_unit, text_unit = refs[:4]
    images = refs[4 : 4 + n_images]
    texts = refs[4 + n_images : 4 + n_images + n_texts]
    send, keep, row_total, col_total, late_text, late_image = refs[4 + n_images + n_texts :]
    rows = images[0].shape[0]
    n_early_images, n_early_texts = early_rows.shape[0], early_cols.shape[0]
    scalars = loss_scalars(scalar_ref)
    for j in range(n_texts):
        late_text[pl.ds(j * rows, rows), :] = unit_rows(texts[j][...])
    losses = pair_losses(scalars, image_unit[...], late_text[...])
    late_sum = col_tile(losses)
    for i in range(n_early_images):
        line = row_line(losses[i * rows : i * rows + rows])
        row_total[i : i + 1, :] = early_rows[i : i + 1, :] + line
    for i in range(n_images):
        late_image[pl.ds(i * rows, rows), :] = unit_rows(images[i][...])
    losses = pair_losses(scalars, late_image[...], late_text[...])
    late_sum = late_sum + col_tile(losses)
    others = pair_losses(scalars, late_image[...], text_unit[...])
    early_sum = col_tile(others)
    for i in range(n_images):
        span, k = slice(i * rows, i * rows + rows), n_early_images + i
        row_total[k : k + 1, :] = row_line(losses[span]) + row_line(others[span])
    for j, line in enumerate(col_lines(early_sum, rows)):
        col_total[j : j + 1, :] = early_cols[j : j + 1, :] + line
    for j, line in enumerate(col_lines(late_sum, rows)):
        k = n_early_texts + j
        col_total[k : k + 1, :] = line
    send[...] = jnp.zeros_like(send)
    keep[...] = jnp.zeros_like(keep)
    row_units, col_units = row_total.shape[0] // 2, col_total.shape[0]

    @pl.when(core[0] == 0)
    def _():
        for m in range(row_units):
            keep[m] = row_total[2 * m : 2 * m + 2, :] * (1.0 / TOK_DEV)
        for m in range(col_units):
            send[m, 1:2] = col_total[m : m + 1, :] * (1.0 / TOK_DEV)

    @pl.when(core[0] != 0)
    def _():
        for m in range(row_units):
            for k in range(2):
                send[m, k : k + 1] = row_total[2 * m + 1 - k : 2 * m + 2 - k, :] * (1.0 / TOK_DEV)
        for m in range(col_units):
            keep[m, 0:1] = col_total[m : m + 1, :] * (1.0 / TOK_DEV)


def estimate(pairs, width, blocks, rows):
    return pl.CostEstimate(
        flops=2 * pairs * width,
        bytes_accessed=blocks * rows * width * 2,
        transcendentals=2 * pairs,
    )


def own_units(log_scale, bias, image, text):
    unit = jax.ShapeDtypeStruct(image.shape, jnp.bfloat16)
    return pl.pallas_call(
        own_kernel,
        out_shape=(jax.ShapeDtypeStruct((2, 128), jnp.float32), unit, unit),
        in_specs=[VMEM] * 4,
        out_specs=(VMEM,) * 3,
        cost_estimate=pl.CostEstimate(
            flops=8 * image.size, bytes_accessed=8 * image.size, transcendentals=0
        ),
        compiler_params=pltpu.CompilerParams(vmem_limit_bytes=16 << 20),
        name="own_units",
    )(log_scale, bias, image, text)


def early_sums(scalars, own_image, own_text, images, texts):
    rows, width = own_image.shape
    n_images, n_texts = len(images) + 1, len(texts) + 1
    return pl.pallas_call(
        lambda *refs: early_kernel(n_images, n_texts, *refs),
        out_shape=(
            jax.ShapeDtypeStruct((n_images, rows), jnp.float32),
            jax.ShapeDtypeStruct((n_texts, rows), jnp.float32),
            jax.ShapeDtypeStruct((n_images * rows, width), jnp.bfloat16),
            jax.ShapeDtypeStruct((n_texts * rows, width), jnp.bfloat16),
        ),
        in_specs=[VMEM] * (1 + n_images + n_texts),
        out_specs=(VMEM,) * 4,
        cost_estimate=estimate(n_images * n_texts * rows * rows, width, n_images + n_texts, rows),
        compiler_params=pltpu.CompilerParams(vmem_limit_bytes=16 << 20),
        name="early_sums",
    )(scalars, own_image, own_text, *images, *texts)


def late_sums(core, scalars, early, images, texts):
    rows, width = images[0].shape
    n_images, n_texts = len(images), len(texts)
    all_images = early[0].shape[0] + n_images
    all_texts = early[1].shape[0] + n_texts
    pairs = (all_images * all_texts - early[0].shape[0] * early[1].shape[0]) * rows * rows
    units = max(all_images // 2, all_texts)
    return pl.pallas_call(
        lambda *refs: late_kernel(n_images, n_texts, *refs),
        out_shape=(jax.ShapeDtypeStruct((units, 2, rows), jnp.float32),) * 2,
        in_specs=[SMEM] + [VMEM] * (5 + n_images + n_texts),
        out_specs=(VMEM, VMEM),
        scratch_shapes=[
            pltpu.VMEM((all_images, rows), jnp.float32),
            pltpu.VMEM((all_texts, rows), jnp.float32),
            pltpu.VMEM((n_texts * rows, width), jnp.bfloat16),
            pltpu.VMEM((n_images * rows, width), jnp.bfloat16),
        ],
        cost_estimate=estimate(pairs, width, all_images + all_texts, rows),
        compiler_params=pltpu.CompilerParams(vmem_limit_bytes=16 << 20),
        name="late_sums",
    )(core, scalars, *early, *images, *texts)


def solution(mesh):
    n_devices = mesh.shape["dp"] * mesh.shape["mp"]
    bits = [1 << k for k in range(int(math.log2(n_devices)))]
    dp_bits = [b for b in bits if b >= mesh.shape["mp"]]
    split = dp_bits[0::2] + dp_bits[1::2]
    text_bits = sorted(split[: len(bits) // 2], reverse=True)
    image_bits = sorted(set(bits) - set(text_bits), reverse=True)
    core_bit, link_bits = image_bits[-1], image_bits[:-1]

    rank = {0: 0}

    def masks_of(order):
        masks = [0]
        for bit in order:
            rank.update({mask ^ bit: rank[mask] + 1 for mask in masks})
            masks = masks + [mask ^ bit for mask in masks]
        return sorted(masks, key=rank.get)

    image_masks = masks_of(link_bits)
    text_masks = masks_of(text_bits)

    def move(value, partner):
        pairs = [(d, partner(d)) for d in range(n_devices) if partner(d) != d]
        return lax.ppermute(value, AXES, pairs)

    def swap(value, bit):
        return move(value, lambda d: d ^ bit)

    def gather(own, order):
        blocks = {0: own}
        for bit in order:
            for mask, block in list(blocks.items()):
                blocks[mask ^ bit] = swap(block, bit)
        return blocks

    def losses(images, texts, log_scale, bias):
        scalars, own_image, own_text = own_units(
            log_scale.reshape(1, 1), bias.reshape(1, 1), images, texts
        )
        core = (lax.axis_index("mp") & 1).astype(jnp.int32)
        image_blocks = {m: move(images, lambda d: d ^ m) for m in image_masks if m}
        image_blocks[0] = images
        text_blocks = gather(texts, text_bits)
        paired = {m: swap(b, core_bit) for m, b in image_blocks.items()}
        early_masks = [m for m in image_masks if rank[m] < 2]
        late_masks = [m for m in image_masks if rank[m] >= 2]
        both = lambda masks: [b for m in masks for b in (image_blocks[m], paired[m])]
        early_texts = [text_blocks[m] for m in text_masks if rank[m] < 2]
        late_texts = [text_blocks[m] for m in text_masks if rank[m] >= 2]
        early = early_sums(
            scalars, own_image, own_text, both(early_masks)[1:], early_texts[1:]
        )
        send, keep = late_sums(
            core.reshape(1), scalars, early, both(late_masks), late_texts
        )
        merged = keep + swap(send, core_bit)
        total = merged[0]
        for k in range(1, merged.shape[0]):
            row_mask = image_masks[k] if k < len(image_masks) else 0
            col_mask = text_masks[k] if k < len(text_masks) else 0
            total = total + move(merged[k], lambda d: d ^ (col_mask if d & core_bit else row_mask))
        other = swap(total[1:2], core_bit)
        on_rows = core == 0
        own = total[0:1]
        row_loss = jnp.where(on_rows, own, other).reshape(-1)
        col_loss = jnp.where(on_rows, other, own).reshape(-1)
        return row_loss, col_loss

    placed = (P(AXES, None), P(AXES, None), P(), P())
    return jax.shard_map(
        losses,
        mesh=mesh,
        in_specs=placed,
        out_specs=(P(AXES), P(AXES)),
        check_vma=False,
    )
```

```python
import math

import jax
import jax.numpy as jnp
from jax import lax
from jax.experimental import pallas as pl
from jax.experimental.pallas import tpu as pltpu
from jax.sharding import PartitionSpec as P

TOK_DEV = 512

EPSILON = 1e-06

LOG2_E = math.log2(math.e)

AXES = ("dp", "mp")


VMEM = pl.BlockSpec(memory_space=pltpu.VMEM)
SMEM = pl.BlockSpec(memory_space=pltpu.SMEM)


def unit_rows(values):
    widened = values.astype(jnp.float32)
    inverse = lax.rsqrt(jnp.sum(widened * widened, axis=1, keepdims=True) + EPSILON)
    return (widened * inverse).astype(jnp.bfloat16)


def softplus(grown):
    series = grown * (1.0 + grown * (-1.0 / 2 + grown * (1.0 / 3)))
    return jnp.where(grown < 1.0 / 64, series, jnp.log(1.0 + grown))


def pair_losses(scalars, image_unit, text_unit, own_pairs=False):
    logit_scale, offset = scalars
    scores = lax.dot_general(
        image_unit, text_unit, (((1,), (1,)), ((), ())), preferred_element_type=jnp.float32
    )
    logits = logit_scale * scores + offset
    if own_pairs:
        down = lax.broadcasted_iota(jnp.int32, logits.shape, 0)
        across = lax.broadcasted_iota(jnp.int32, logits.shape, 1)
        logits = jnp.where(down == across, -logits, logits)
    return softplus(jnp.exp2(logits))


def row_line(losses):
    rows = losses.shape[0]
    lanes = [losses[:, k : k + rows] for k in range(0, losses.shape[1], rows)]
    return jnp.sum(sum(lanes[1:], lanes[0]).T, axis=0, keepdims=True)


def col_tile(losses):
    return jnp.sum(losses.reshape(losses.shape[0] // 8, 8, losses.shape[1]), axis=0)


def col_lines(tile, rows):
    line = jnp.sum(tile, axis=0, keepdims=True)
    return [line[:, k : k + rows] for k in range(0, line.shape[1], rows)]


def own_kernel(log_scale, bias, image, text, scalars, image_unit, text_unit):
    line = scalars.shape[1]
    scalars[0:1, :] = jnp.broadcast_to(jnp.exp(log_scale[...]) * LOG2_E, (1, line))
    scalars[1:2, :] = jnp.broadcast_to(bias[...] * LOG2_E, (1, line))
    image_unit[...] = unit_rows(image[...])
    text_unit[...] = unit_rows(text[...])


def loss_scalars(ref):
    return ref[0:1, 0:1], ref[1:2, 0:1]


def early_kernel(n_images, n_texts, scalar_ref, own_image, own_text, *refs):
    images = (own_image,) + refs[: n_images - 1]
    texts = (own_text,) + refs[n_images - 1 : n_images + n_texts - 2]
    row_out, col_out, image_unit, text_unit = refs[n_images + n_texts - 2 :]
    rows = own_image.shape[0]
    scalars = loss_scalars(scalar_ref)
    for j in range(n_texts):
        unit = unit_rows(texts[j][...]) if j else own_text[...]
        text_unit[pl.ds(j * rows, rows), :] = unit
    col_sum = None
    for i in range(n_images):
        unit = unit_rows(images[i][...]) if i else own_image[...]
        image_unit[pl.ds(i * rows, rows), :] = unit
        losses = pair_losses(scalars, unit, text_unit[...], own_pairs=i == 0)
        row_out[i : i + 1, :] = row_line(losses)
        tile = col_tile(losses)
        col_sum = tile if col_sum is None else col_sum + tile
    for j, line in enumerate(col_lines(col_sum, rows)):
        col_out[j : j + 1, :] = line


def middle_kernel(n_images, scalar_ref, early_cols, text_unit, *refs):
    images, (row_out, col_out, image_unit) = refs[:n_images], refs[n_images:]
    rows = images[0].shape[0]
    scalars = loss_scalars(scalar_ref)
    for i in range(n_images):
        image_unit[pl.ds(i * rows, rows), :] = unit_rows(images[i][...])
    losses = pair_losses(scalars, image_unit[...], text_unit[...])
    for i in range(n_images):
        row_out[i : i + 1, :] = row_line(losses[i * rows : i * rows + rows])
    for j, line in enumerate(col_lines(col_tile(losses), rows)):
        col_out[j : j + 1, :] = early_cols[j : j + 1, :] + line


def late_kernel(n_images, n_texts, core, scalar_ref, *refs):
    early_rows, image_unit, text_unit, middle_rows, early_cols, middle_unit = refs[:6]
    images = refs[6 : 6 + n_images]
    texts = refs[6 + n_images : 6 + n_images + n_texts]
    send, keep, row_total, col_total, late_text, late_image = refs[6 + n_images + n_texts :]
    rows = images[0].shape[0]
    n_early_images, n_early_texts = early_rows.shape[0], early_cols.shape[0]
    scalars = loss_scalars(scalar_ref)
    for j in range(n_texts):
        late_text[pl.ds(j * rows, rows), :] = unit_rows(texts[j][...])
    losses = pair_losses(scalars, image_unit[...], late_text[...])
    late_sum = col_tile(losses)
    for i in range(n_early_images):
        line = row_line(losses[i * rows : i * rows + rows])
        row_total[i : i + 1, :] = early_rows[i : i + 1, :] + line
    half = n_images * rows
    late_image[pl.ds(0, half), :] = middle_unit[...]
    for i in range(n_images):
        late_image[pl.ds(half + i * rows, rows), :] = unit_rows(images[i][...])
    losses = pair_losses(scalars, late_image[...], late_text[...])
    late_sum = late_sum + col_tile(losses)
    others = pair_losses(scalars, late_image[pl.ds(half, half), :], text_unit[...])
    early_sum = col_tile(others)
    for i in range(n_images):
        span, k = slice(i * rows, i * rows + rows), n_early_images + 2 * i
        row_total[k : k + 1, :] = middle_rows[i : i + 1, :] + row_line(losses[span])
        after = losses[half + i * rows : half + i * rows + rows]
        row_total[k + 1 : k + 2, :] = row_line(after) + row_line(others[span])
    for j, line in enumerate(col_lines(early_sum, rows)):
        col_total[j : j + 1, :] = early_cols[j : j + 1, :] + line
    for j, line in enumerate(col_lines(late_sum, rows)):
        k = n_early_texts + j
        col_total[k : k + 1, :] = line
    send[...] = jnp.zeros_like(send)
    keep[...] = jnp.zeros_like(keep)
    row_units, col_units = row_total.shape[0] // 2, col_total.shape[0]

    @pl.when(core[0] == 0)
    def _():
        for m in range(row_units):
            keep[m] = row_total[2 * m : 2 * m + 2, :] * (1.0 / TOK_DEV)
        for m in range(col_units):
            send[m, 1:2] = col_total[m : m + 1, :] * (1.0 / TOK_DEV)

    @pl.when(core[0] != 0)
    def _():
        for m in range(row_units):
            for k in range(2):
                send[m, k : k + 1] = row_total[2 * m + 1 - k : 2 * m + 2 - k, :] * (1.0 / TOK_DEV)
        for m in range(col_units):
            keep[m, 0:1] = col_total[m : m + 1, :] * (1.0 / TOK_DEV)


def estimate(pairs, width, blocks, rows):
    return pl.CostEstimate(
        flops=2 * pairs * width,
        bytes_accessed=blocks * rows * width * 2,
        transcendentals=2 * pairs,
    )


def own_units(log_scale, bias, image, text):
    unit = jax.ShapeDtypeStruct(image.shape, jnp.bfloat16)
    return pl.pallas_call(
        own_kernel,
        out_shape=(jax.ShapeDtypeStruct((2, 128), jnp.float32), unit, unit),
        in_specs=[VMEM] * 4,
        out_specs=(VMEM,) * 3,
        cost_estimate=pl.CostEstimate(
            flops=8 * image.size, bytes_accessed=8 * image.size, transcendentals=0
        ),
        compiler_params=pltpu.CompilerParams(vmem_limit_bytes=16 << 20),
        name="own_units",
    )(log_scale, bias, image, text)


def early_sums(scalars, own_image, own_text, images, texts):
    rows, width = own_image.shape
    n_images, n_texts = len(images) + 1, len(texts) + 1
    return pl.pallas_call(
        lambda *refs: early_kernel(n_images, n_texts, *refs),
        out_shape=(
            jax.ShapeDtypeStruct((n_images, rows), jnp.float32),
            jax.ShapeDtypeStruct((n_texts, rows), jnp.float32),
            jax.ShapeDtypeStruct((n_images * rows, width), jnp.bfloat16),
            jax.ShapeDtypeStruct((n_texts * rows, width), jnp.bfloat16),
        ),
        in_specs=[VMEM] * (1 + n_images + n_texts),
        out_specs=(VMEM,) * 4,
        cost_estimate=estimate(n_images * n_texts * rows * rows, width, n_images + n_texts, rows),
        compiler_params=pltpu.CompilerParams(vmem_limit_bytes=16 << 20),
        name="early_sums",
    )(scalars, own_image, own_text, *images, *texts)


def middle_sums(scalars, early, images):
    rows, width = images[0].shape
    n_images = len(images)
    lines = [jax.ShapeDtypeStruct((n, rows), jnp.float32) for n in (n_images, early[1].shape[0])]
    return pl.pallas_call(
        lambda *refs: middle_kernel(n_images, *refs),
        out_shape=(*lines, jax.ShapeDtypeStruct((n_images * rows, width), jnp.bfloat16)),
        in_specs=[VMEM] * (3 + n_images),
        out_specs=(VMEM,) * 3,
        cost_estimate=estimate(n_images * early[1].shape[0] * rows * rows, width, n_images, rows),
        compiler_params=pltpu.CompilerParams(vmem_limit_bytes=16 << 20),
        name="middle_sums",
    )(scalars, early[1], early[3], *images)


def late_sums(core, scalars, early, middle, images, texts):
    rows, width = images[0].shape
    n_images, n_texts = len(images), len(texts)
    all_images = early[0].shape[0] + 2 * n_images
    all_texts = early[1].shape[0] + n_texts
    pairs = (all_images * all_texts - early[0].shape[0] * early[1].shape[0]) * rows * rows
    units = max(all_images // 2, all_texts)
    return pl.pallas_call(
        lambda *refs: late_kernel(n_images, n_texts, *refs),
        out_shape=(jax.ShapeDtypeStruct((units, 2, rows), jnp.float32),) * 2,
        in_specs=[SMEM] + [VMEM] * (7 + n_images + n_texts),
        out_specs=(VMEM, VMEM),
        scratch_shapes=[
            pltpu.VMEM((all_images, rows), jnp.float32),
            pltpu.VMEM((all_texts, rows), jnp.float32),
            pltpu.VMEM((n_texts * rows, width), jnp.bfloat16),
            pltpu.VMEM((2 * n_images * rows, width), jnp.bfloat16),
        ],
        cost_estimate=estimate(pairs, width, all_images + all_texts, rows),
        compiler_params=pltpu.CompilerParams(vmem_limit_bytes=16 << 20),
        name="late_sums",
    )(core, scalars, early[0], early[2], early[3], *middle, *images, *texts)


def solution(mesh):
    n_devices = mesh.shape["dp"] * mesh.shape["mp"]
    bits = [1 << k for k in range(int(math.log2(n_devices)))]
    dp_bits = [b for b in bits if b >= mesh.shape["mp"]]
    split = dp_bits[0::2] + dp_bits[1::2]
    text_bits = sorted(split[: len(bits) // 2], reverse=True)
    image_bits = sorted(set(bits) - set(text_bits), reverse=True)
    core_bit, link_bits = image_bits[-1], image_bits[:-1]

    rank = {0: 0}

    def masks_of(order):
        masks = [0]
        for bit in order:
            rank.update({mask ^ bit: rank[mask] + 1 for mask in masks})
            masks = masks + [mask ^ bit for mask in masks]
        return sorted(masks, key=rank.get)

    image_masks = masks_of(link_bits)
    text_masks = masks_of(text_bits)

    def move(value, partner):
        pairs = [(d, partner(d)) for d in range(n_devices) if partner(d) != d]
        return lax.ppermute(value, AXES, pairs)

    def swap(value, bit):
        return move(value, lambda d: d ^ bit)

    def gather(own, order):
        blocks = {0: own}
        for bit in order:
            for mask, block in list(blocks.items()):
                blocks[mask ^ bit] = swap(block, bit)
        return blocks

    def losses(images, texts, log_scale, bias):
        scalars, own_image, own_text = own_units(
            log_scale.reshape(1, 1), bias.reshape(1, 1), images, texts
        )
        core = (lax.axis_index("mp") & 1).astype(jnp.int32)
        image_blocks = {m: move(images, lambda d: d ^ m) for m in image_masks if m}
        image_blocks[0] = images
        text_blocks = gather(texts, text_bits)
        paired = {m: swap(b, core_bit) for m, b in image_blocks.items()}
        early_masks = [m for m in image_masks if rank[m] < 2]
        late_masks = [m for m in image_masks if rank[m] >= 2]
        both = lambda masks: [b for m in masks for b in (image_blocks[m], paired[m])]
        early_texts = [text_blocks[m] for m in text_masks if rank[m] < 2]
        late_texts = [text_blocks[m] for m in text_masks if rank[m] >= 2]
        early = early_sums(
            scalars, own_image, own_text, both(early_masks)[1:], early_texts[1:]
        )
        middle = middle_sums(scalars, early, [image_blocks[m] for m in late_masks])
        send, keep = late_sums(
            core.reshape(1), scalars, early, middle, [paired[m] for m in late_masks], late_texts
        )
        merged = keep + swap(send, core_bit)
        total = merged[0]
        for k in range(1, merged.shape[0]):
            row_mask = image_masks[k] if k < len(image_masks) else 0
            col_mask = text_masks[k] if k < len(text_masks) else 0
            total = total + move(merged[k], lambda d: d ^ (col_mask if d & core_bit else row_mask))
        other = swap(total[1:2], core_bit)
        on_rows = core == 0
        own = total[0:1]
        row_loss = jnp.where(on_rows, own, other).reshape(-1)
        col_loss = jnp.where(on_rows, other, own).reshape(-1)
        return row_loss, col_loss

    placed = (P(AXES, None), P(AXES, None), P(), P())
    return jax.shard_map(
        losses,
        mesh=mesh,
        in_specs=placed,
        out_specs=(P(AXES), P(AXES)),
        check_vma=False,
    )
```
